64 devices in a mesh: data: 4 (over x, y), time: 16 (over z, core).
Axes of the slice: x: 2, y: 2, z: 8, core: 2. Of those that a mesh axis runs over, the one named last changes fastest.
The devices are a block of a 4x4x8 slice.
Arguments:
- x_init: float32 [32, 1024, 16], P('data'), parts along dimension 0
- w_in: bfloat16 [16, 1152], replicated
- w_out: bfloat16 [1152, 16], replicated
- mod_scale: bfloat16 [16, 1152], P('time')
- mod_shift: bfloat16 [16, 1152], P('time')
- step_size: float32 [16], P('time')
Outputs:
- output: float32 [16, 32, 1024, 16], P('time', 'data'), parts along dimension 1
There are 4 independent parts. The reference program is written for one: setup_inputs(seed, part) draws one part's arguments, and reference() takes and returns one part's arrays. A program takes and returns all parts, laid end to end along the dimension named above; an argument that names none is the same for every part.
All inputs are finite; a program needn't handle non-finite values.
Results may differ from the reference program's by a relative error of at most 0.001.
Values are sent between devices in bfloat16 or wider.
A program may use at most 768 MiB of HBM per device.

```python
import jax
import jax.numpy as jnp
from jax import lax

BATCH = 8
TOKENS = 1024
CHANNELS = 16
HIDDEN = 1152
STEPS = 16
SWEEPS = 4


def setup_inputs(seed: int = 0, part: int = 0) -> dict:
    key_list = jax.random.split(jax.random.key(seed), 7)
    x_init = jax.random.normal(jax.random.fold_in(key_list[0], part), (BATCH, TOKENS, CHANNELS), jnp.float32)
    w_in = jax.random.normal(key_list[1], (CHANNELS, HIDDEN), jnp.float32) * (CHANNELS * STEPS) ** -0.5
    w_raw = jax.random.normal(key_list[2], (HIDDEN, CHANNELS), jnp.float32)
    w_out = (w_raw - jnp.mean(w_raw, axis=0, keepdims=True)) * (1.5 * HIDDEN ** -0.5)
    time_pos = (jnp.arange(STEPS, dtype=jnp.float32) + 0.5) / STEPS
    mode_coef = 0.4 * jax.random.normal(key_list[3], (3, HIDDEN), jnp.float32)
    mod_scale = (mode_coef[0][None, :] + mode_coef[1][None, :] * jnp.cos(jnp.pi * time_pos)[:, None] + mode_coef[2][None, :] * jnp.cos(2.0 * jnp.pi * time_pos)[:, None] + 0.1 * jax.random.normal(key_list[4], (STEPS, HIDDEN), jnp.float32))
    mod_shift = jax.random.normal(key_list[5], (STEPS, HIDDEN), jnp.float32)
    step_size = jax.random.uniform(key_list[6], (STEPS,), jnp.float32, 0.5, 1.5) * STEPS ** -0.5
    return {"x_init": x_init, "w_in": w_in.astype(jnp.bfloat16), "w_out": w_out.astype(jnp.bfloat16), "mod_scale": mod_scale.astype(jnp.bfloat16), "mod_shift": mod_shift.astype(jnp.bfloat16), "step_size": step_size}


def denoise(latent, w_in, w_out, scale_row, shift_row):
    flat_in = latent.astype(jnp.bfloat16).reshape(-1, latent.shape[-1])
    pre_act = jnp.dot(flat_in, w_in, preferred_element_type=jnp.float32)
    hidden_act = jax.nn.gelu(pre_act * (1.0 + scale_row.astype(jnp.float32)) + shift_row.astype(jnp.float32), approximate=True)
    return jnp.dot(hidden_act.astype(jnp.bfloat16), w_out, preferred_element_type=jnp.float32).reshape(latent.shape)


def reference(x_init, w_in, w_out, mod_scale, mod_shift, step_size):
    def one_step_drift(item):
        return denoise(item[0], w_in, w_out, item[1], item[2])

    def one_sweep(latents, unused):
        drifts = lax.map(one_step_drift, (latents, mod_scale, mod_shift))
        increments = step_size[:-1, None, None, None] * (0.5 * (drifts[:-1] + drifts[1:]))
        running = jnp.cumsum(increments, axis=0)
        return jnp.concatenate([x_init[None], x_init[None] + running], axis=0), unused

    start = jnp.broadcast_to(x_init[None], (STEPS,) + x_init.shape)
    final, unused_out = lax.scan(one_sweep, start, None, length=SWEEPS)
    return final
```

```python
import functools

import jax
import jax.numpy as jnp
from jax import lax
from jax.experimental import pallas as pl
from jax.experimental.pallas import tpu as pltpu
from jax.sharding import PartitionSpec as P

SWEEPS = 4
TANH_LIN = 0.7978845608028654
TANH_CUB = TANH_LIN * 0.044715
CHUNK = 256
BLOCK = 384
LEAD = 1
LAG = 1


def half_gelu_arg(half):
    square = half * half
    poly = square * (8.0 * TANH_CUB) + 2.0 * TANH_LIN
    gate = jnp.tanh(half * poly)
    return (half * (1.0 + gate)).astype(jnp.bfloat16)


def kernel_body(n_time, x_ref, w_in_ref, w_out_ref, scale_ref, shift_ref, step_ref, out_ref,
                scale_all, shift_all, step_all, weights, x_mine, x_half, d_first, x_out,
                local_sem, mod_send, mod_recv, out_send, out_recv):
    me = lax.axis_index("time")
    channels, hidden = w_in_ref.shape
    batch, _, tokens = x_ref.shape
    mine = batch * tokens // n_time
    per_row = tokens // mine
    n_chunks = mine // CHUNK

    def spot(device):
        return lax.div(device, per_row), lax.rem(device, per_row) * mine

    my_row, my_off = spot(me)
    fetch = pltpu.make_async_copy(x_ref.at[my_row, :, pl.ds(pl.multiple_of(my_off, mine), mine)], x_mine, local_sem.at[0])
    fetch.start()

    barrier = pltpu.get_barrier_semaphore()
    for dist in range(1, n_time):
        pl.semaphore_signal(barrier, inc=1, device_id={"time": lax.rem(me + dist, n_time)}, device_id_type=pl.DeviceIdType.MESH)

    step_all[me] = jnp.full(step_all.shape[1:], step_ref[0], jnp.float32)
    scale_all[me] = scale_ref[...]
    shift_all[me] = shift_ref[...]
    pl.semaphore_wait(barrier, n_time - 1)

    def mod_copies(source, target, slot):
        return [
            pltpu.make_async_remote_copy(src_ref=src, dst_ref=dst.at[source], send_sem=mod_send.at[kind, slot], recv_sem=mod_recv.at[kind, source],
                                         device_id={"time": target}, device_id_type=pl.DeviceIdType.MESH)
            for kind, (src, dst) in enumerate(((scale_ref, scale_all), (shift_ref, shift_all), (step_all.at[me], step_all)))
        ]

    for dist in range(1, n_time):
        for copy in mod_copies(me, lax.rem(me + dist, n_time), dist):
            copy.start()
    fetch.wait()

    @pl.when(me == 0)
    def _():
        whole = pltpu.make_async_copy(x_ref, out_ref, local_sem.at[1])
        whole.start()
        whole.wait()

    for dist in range(1, n_time):
        source = lax.rem(me + dist, n_time)
        for copy in mod_copies(source, source, dist):
            copy.wait_recv()

    w_wide = w_in_ref[...].astype(jnp.float32)

    def prepare(step, carry):
        folded = w_wide * (0.5 * (1.0 + scale_all[step].astype(jnp.float32)))
        high = folded.astype(jnp.bfloat16).astype(jnp.float32)
        rest = folded - high
        middle = rest.astype(jnp.bfloat16).astype(jnp.float32)
        low = rest - middle
        first_row = lax.broadcasted_iota(jnp.int32, (channels, hidden), 0) == 0
        bias = jnp.where(first_row, jnp.broadcast_to(0.5 * shift_all[step].astype(jnp.float32), (channels, hidden)), 0.0)
        stack = jnp.concatenate([high, middle, low, bias], axis=0)
        weights[step] = stack.T.astype(jnp.bfloat16)
        return carry

    lax.fori_loop(0, n_time, prepare, 0)

    ones = jnp.ones((channels, CHUNK), jnp.bfloat16)
    n_blocks = hidden // BLOCK

    def evaluate(steps, get_x, put):
        blocks = [(step, block) for step in steps for block in range(n_blocks)]
        stacked, pre, act, drift = {}, {}, {}, {}

        def project(index):
            step, block = blocks[index]
            if step not in stacked:
                x = get_x(step)
                stacked[step] = jnp.concatenate([x, x, x, ones], axis=0)
            pre[index] = jnp.dot(weights[step, block * BLOCK:(block + 1) * BLOCK, :], stacked[step], preferred_element_type=jnp.float32)

        def contract(index):
            step, block = blocks[index]
            part = jnp.dot(w_out_ref[:, block * BLOCK:(block + 1) * BLOCK], act.pop(index), preferred_element_type=jnp.float32)
            drift[step] = part if block == 0 else drift[step] + part
            if block == n_blocks - 1:
                put(step, drift.pop(step))

        for index in range(len(blocks) + LEAD + LAG):
            if index < len(blocks):
                project(index)
            if LEAD <= index < len(blocks) + LEAD:
                act[index - LEAD] = half_gelu_arg(pre.pop(index - LEAD))
            if index >= LEAD + LAG:
                contract(index - LEAD - LAG)

    def out_copy(chunk, source, target):
        row, off = spot(source)
        cols = pl.ds(pl.multiple_of(off + chunk * CHUNK, CHUNK), CHUNK)
        return pltpu.make_async_remote_copy(
            src_ref=x_out.at[chunk, target], dst_ref=out_ref.at[row, :, cols], send_sem=out_send.at[chunk, target],
            recv_sem=out_recv.at[chunk, source], device_id={"time": target}, device_id_type=pl.DeviceIdType.MESH)

    def run_chunk(chunk, carry):
        start = x_mine[:, pl.ds(pl.multiple_of(chunk * CHUNK, CHUNK), CHUNK)]
        start_half = start.astype(jnp.bfloat16)
        for step in range(1, n_time):
            x_half[step] = start_half

        def put_first(step, drift):
            d_first[...] = drift

        evaluate([0], lambda step: start_half, put_first)

        def sweep(index, carry):
            state = {"last": d_first[...], "x": start}

            def put(step, drift):
                state["x"] = state["x"] + step_all[step - 1] * (0.5 * (state["last"] + drift))
                state["last"] = drift
                x_half[step] = state["x"].astype(jnp.bfloat16)
                x_out[chunk, step] = state["x"]

            evaluate(list(range(1, n_time)), lambda step: x_half[step], put)
            return carry

        lax.fori_loop(0, SWEEPS, sweep, 0)
        for target in range(1, n_time):
            @pl.when(me != target)
            def _():
                out_copy(chunk, me, target).start()

            @pl.when(me == target)
            def _():
                out_ref[my_row, :, pl.ds(pl.multiple_of(my_off + chunk * CHUNK, CHUNK), CHUNK)] = x_out[chunk, target]
        return carry

    lax.fori_loop(0, n_chunks, run_chunk, 0)

    for dist in range(1, n_time):
        for copy in mod_copies(me, lax.rem(me + dist, n_time), dist):
            copy.wait_send()
    for chunk in range(n_chunks):
        for target in range(1, n_time):
            @pl.when(me != target)
            def _():
                out_copy(chunk, me, target).wait_send()

    @pl.when(me != 0)
    def _():
        for chunk in range(n_chunks):
            for dist in range(1, n_time):
                out_copy(chunk, lax.rem(me + dist, n_time), me).wait_recv()


def solution(mesh):
    n_time = mesh.shape["time"]

    def local(x_init, w_in, w_out, mod_scale, mod_shift, step_size):
        batch, tokens, channels = x_init.shape
        hidden = w_in.shape[1]
        mine = batch * tokens // n_time
        n_chunks = mine // CHUNK
        vmem = pl.BlockSpec(memory_space=pltpu.VMEM)
        out = pl.pallas_call(
            functools.partial(kernel_body, n_time),
            out_shape=jax.ShapeDtypeStruct((batch, channels, tokens), jnp.float32),
            in_specs=[pl.BlockSpec(memory_space=pl.ANY), vmem, vmem, vmem, vmem, pl.BlockSpec(memory_space=pltpu.SMEM)],
            out_specs=vmem,
            scratch_shapes=[
                pltpu.VMEM((n_time, 1, hidden), jnp.bfloat16),
                pltpu.VMEM((n_time, 1, hidden), jnp.bfloat16),
                pltpu.VMEM((n_time, 1, CHUNK), jnp.float32),
                pltpu.VMEM((n_time, hidden, 4 * channels), jnp.bfloat16),
                pltpu.VMEM((channels, mine), jnp.float32),
                pltpu.VMEM((n_time, channels, CHUNK), jnp.bfloat16),
                pltpu.VMEM((channels, CHUNK), jnp.float32),
                pltpu.VMEM((n_chunks, n_time, channels, CHUNK), jnp.float32),
                pltpu.SemaphoreType.DMA((2,)),
                pltpu.SemaphoreType.DMA((3, n_time)),
                pltpu.SemaphoreType.DMA((3, n_time)),
                pltpu.SemaphoreType.DMA((n_chunks, n_time)),
                pltpu.SemaphoreType.DMA((n_chunks, n_time)),
            ],
            compiler_params=pltpu.CompilerParams(collective_id=0, has_side_effects=True, vmem_limit_bytes=48 * 2**20),
            name="picard",
        )(jnp.swapaxes(x_init, 1, 2), w_in, w_out.T, mod_scale, mod_shift, step_size)
        return jnp.swapaxes(out, 1, 2)[None]

    return jax.shard_map(local, mesh=mesh, in_specs=(P("data"), P(), P(), P("time"), P("time"), P("time")), out_specs=P("time", "data"), check_vma=False)
```

```python
import functools

import jax
import jax.numpy as jnp
from jax import lax
from jax.experimental import pallas as pl
from jax.experimental.pallas import tpu as pltpu
from jax.sharding import PartitionSpec as P

SWEEPS = 4
TANH_LIN = 0.7978845608028654
TANH_CUB = TANH_LIN * 0.044715
CHUNK = 256
BLOCK = 384
LEAD = 1
LAG = 1
SEND_AFTER = (8, 13)


def half_gelu_arg(half):
    square = half * half
    poly = square * (8.0 * TANH_CUB) + 2.0 * TANH_LIN
    gate = jnp.tanh(half * poly)
    return (half * (1.0 + gate)).astype(jnp.bfloat16)


def kernel_body(n_time, x_ref, w_in_ref, w_out_ref, scale_ref, shift_ref, step_ref, out_ref,
                w_in, w_out, step_own, scale_all, shift_all, step_all, weights, x_mine, x_half, drifts, x_out,
                local_sem, whole_sem, mod_send, mod_recv, out_send, out_recv):
    me = lax.axis_index("time")
    channels, hidden = w_in.shape
    batch, _, tokens = x_ref.shape
    mine = batch * tokens // n_time
    per_row = tokens // mine
    n_chunks = mine // CHUNK
    n_blocks = hidden // BLOCK
    n_chips = n_time // 2

    def spot(device):
        return lax.div(device, per_row), lax.rem(device, per_row) * mine

    my_row, my_off = spot(me)
    fetches = [
        pltpu.make_async_copy(src, dst, local_sem.at[slot])
        for slot, (src, dst) in enumerate((
            (scale_ref, scale_all.at[me]), (shift_ref, shift_all.at[me]), (step_ref, step_own), (w_in_ref, w_in), (w_out_ref, w_out),
            (x_ref.at[my_row, :, pl.ds(pl.multiple_of(my_off, mine), mine)], x_mine)))
    ]
    for fetch in fetches:
        fetch.start()

    chip, core = lax.div(me, 2), lax.rem(me, 2)

    def peer_of(slot):
        return lax.rem(chip + slot // 2, n_chips) * 2 + lax.rem(core + slot % 2, 2)

    def slot_of(step):
        return lax.rem(step // 2 + n_chips - chip, n_chips) * 2 + lax.rem(step % 2 + 2 - core, 2)

    groups = [[1]]
    for dist in range(1, n_chips // 2 + 1):
        ways = (dist,) if 2 * dist == n_chips else (dist, n_chips - dist)
        groups.append([way * 2 + other for way in ways for other in range(2)])
    near_first = [slot for group in groups for slot in group]

    barrier = pltpu.get_barrier_semaphore()
    for slot in reversed(near_first):
        pl.semaphore_signal(barrier, inc=1, device_id={"time": peer_of(slot)}, device_id_type=pl.DeviceIdType.MESH)
    for fetch in fetches:
        fetch.wait()
    step_all[me] = jnp.full(step_all.shape[1:], step_own[0], jnp.float32)

    @pl.when(me == 0)
    def _():
        pltpu.make_async_copy(x_ref, out_ref, whole_sem.at[0]).start()

    def mod_copies(source, target, slot):
        return [
            pltpu.make_async_remote_copy(src_ref=ref.at[source], dst_ref=ref.at[source], send_sem=mod_send.at[kind, slot], recv_sem=mod_recv.at[kind, source],
                                         device_id={"time": target}, device_id_type=pl.DeviceIdType.MESH)
            for kind, ref in enumerate((scale_all, shift_all, step_all))
        ]

    def prepare(slot):
        step = peer_of(slot)
        folded = w_in[...].astype(jnp.float32) * (0.5 * (1.0 + scale_all[step].astype(jnp.float32)))
        high = folded.astype(jnp.bfloat16).astype(jnp.float32)
        rest = folded - high
        middle = rest.astype(jnp.bfloat16).astype(jnp.float32)
        low = rest - middle
        first_row = lax.broadcasted_iota(jnp.int32, (channels, hidden), 0) == 0
        bias = jnp.where(first_row, jnp.broadcast_to(0.5 * shift_all[step].astype(jnp.float32), (channels, hidden)), 0.0)
        stack = jnp.concatenate([high, middle, low, bias], axis=0)
        weights[slot] = stack.T.astype(jnp.bfloat16)

    ones = jnp.ones((channels, CHUNK), jnp.bfloat16)

    def evaluate(items, extras=()):
        extras = list(extras)
        blocks = [(item, block) for item in range(len(items)) for block in range(n_blocks)]
        every = max(1, len(blocks) // max(1, len(extras)))
        stacked, pre, act, drift = {}, {}, {}, {}

        def project(index):
            item, block = blocks[index]
            slot, get_x, _ = items[item]
            if item not in stacked:
                x = get_x()
                stacked[item] = jnp.concatenate([x, x, x, ones], axis=0)
            pre[index] = jnp.dot(weights[slot, block * BLOCK:(block + 1) * BLOCK, :], stacked[item], preferred_element_type=jnp.float32)

        def contract(index):
            item, block = blocks[index]
            part = jnp.dot(w_out[:, block * BLOCK:(block + 1) * BLOCK], act.pop(index), preferred_element_type=jnp.float32)
            drift[item] = part if block == 0 else drift[item] + part
            if block == n_blocks - 1:
                items[item][2](drift.pop(item))

        for index in range(len(blocks) + LEAD + LAG):
            if index < len(blocks):
                project(index)
                if extras and index % every == 0:
                    extras.pop(0)()
            if LEAD <= index < len(blocks) + LEAD:
                act[index - LEAD] = half_gelu_arg(pre.pop(index - LEAD))
            if index >= LEAD + LAG:
                contract(index - LEAD - LAG)
        for extra in extras:
            extra()

    def columns(chunk):
        return pl.ds(pl.multiple_of(chunk * CHUNK, CHUNK), CHUNK)

    def first_items(slots):
        def item(slot, chunk):
            def put(drift):
                drifts[slot, chunk] = drift
            return slot, lambda: x_mine[:, columns(chunk)].astype(jnp.bfloat16), put
        return [item(slot, chunk) for slot in slots for chunk in range(n_chunks)]

    prepare(0)
    pl.semaphore_wait(barrier, n_time - 1)
    for slot in near_first:
        for copy in mod_copies(me, peer_of(slot), slot):
            copy.start()

    evaluate(first_items([0]))
    ready = []
    for arrival in (groups[0] + groups[1], groups[2], [slot for group in groups[3:] for slot in group]):
        for slot in arrival:
            for copy in mod_copies(peer_of(slot), peer_of(slot), slot):
                copy.wait_recv()
        evaluate(first_items(ready), [functools.partial(prepare, slot) for slot in arrival])
        ready = arrival
    evaluate(first_items(ready))

    def integrate(chunk):
        last, x = drifts[slot_of(0), chunk], x_mine[:, columns(chunk)]
        for step in range(1, n_time):
            drift = drifts[slot_of(step), chunk]
            x = x + step_all[step - 1] * (0.5 * (last + drift))
            last = drift
            x_half[step] = x.astype(jnp.bfloat16)

    def out_copy(chunk, source, target):
        row, off = spot(source)
        cols = pl.ds(pl.multiple_of(off + chunk * CHUNK, CHUNK), CHUNK)
        return pltpu.make_async_remote_copy(
            src_ref=x_out.at[chunk, target], dst_ref=out_ref.at[row, :, cols], send_sem=out_send.at[chunk, target],
            recv_sem=out_recv.at[chunk, source], device_id={"time": target}, device_id_type=pl.DeviceIdType.MESH)

    def sweep_items(chunk, steps, state, keep):
        def item(step):
            def put(drift):
                state["x"] = state["x"] + step_all[step - 1] * (0.5 * (state["last"] + drift))
                state["last"] = drift
                if keep:
                    x_out[chunk, step] = state["x"]
                else:
                    x_half[step] = state["x"].astype(jnp.bfloat16)
            return slot_of(step), lambda: x_half[step], put
        return [item(step) for step in steps]

    def run_chunk(chunk, carry):
        integrate(chunk)

        def sweep(index, carry):
            state = {"last": drifts[slot_of(0), chunk], "x": x_mine[:, columns(chunk)]}
            evaluate(sweep_items(chunk, range(1, n_time), state, False))
            return carry

        lax.fori_loop(1, SWEEPS - 1, sweep, 0)
        state = {"last": drifts[slot_of(0), chunk], "x": x_mine[:, columns(chunk)]}
        begin = 1
        for end in SEND_AFTER + (n_time,):
            evaluate(sweep_items(chunk, range(begin, end), state, True))
            for target in range(begin, end):
                @pl.when(me != target)
                def _():
                    out_copy(chunk, me, target).start()
            begin = end

        @pl.when(me != 0)
        def _():
            out_ref[my_row, :, pl.ds(pl.multiple_of(my_off + chunk * CHUNK, CHUNK), CHUNK)] = x_out[chunk, me]
        return carry

    lax.fori_loop(0, n_chunks, run_chunk, 0)

    for slot in near_first:
        for copy in mod_copies(me, peer_of(slot), slot):
            copy.wait_send()

    @pl.when(me == 0)
    def _():
        pltpu.make_async_copy(x_ref, out_ref, whole_sem.at[0]).wait()

    for chunk in range(n_chunks):
        for target in range(1, n_time):
            @pl.when(me != target)
            def _():
                out_copy(chunk, me, target).wait_send()

    @pl.when(me != 0)
    def _():
        for chunk in range(n_chunks):
            for dist in range(1, n_time):
                out_copy(chunk, lax.rem(me + dist, n_time), me).wait_recv()


def solution(mesh):
    n_time = mesh.shape["time"]

    def local(x_init, w_in, w_out, mod_scale, mod_shift, step_size):
        batch, tokens, channels = x_init.shape
        hidden = w_in.shape[1]
        mine = batch * tokens // n_time
        n_chunks = mine // CHUNK
        out = pl.pallas_call(
            functools.partial(kernel_body, n_time),
            out_shape=jax.ShapeDtypeStruct((batch, channels, tokens), jnp.float32),
            in_specs=[pl.BlockSpec(memory_space=pltpu.HBM)] * 6,
            out_specs=pl.BlockSpec(memory_space=pltpu.VMEM),
            scratch_shapes=[
                pltpu.VMEM((channels, hidden), jnp.bfloat16),
                pltpu.VMEM((channels, hidden), jnp.bfloat16),
                pltpu.SMEM((1,), jnp.float32),
                pltpu.VMEM((n_time, 1, hidden), jnp.bfloat16),
                pltpu.VMEM((n_time, 1, hidden), jnp.bfloat16),
                pltpu.VMEM((n_time, 1, CHUNK), jnp.float32),
                pltpu.VMEM((n_time, hidden, 4 * channels), jnp.bfloat16),
                pltpu.VMEM((channels, mine), jnp.float32),
                pltpu.VMEM((n_time, channels, CHUNK), jnp.bfloat16),
                pltpu.VMEM((n_time, n_chunks, channels, CHUNK), jnp.float32),
                pltpu.VMEM((n_chunks, n_time, channels, CHUNK), jnp.float32),
                pltpu.SemaphoreType.DMA((6,)),
                pltpu.SemaphoreType.DMA((1,)),
                pltpu.SemaphoreType.DMA((3, n_time)),
                pltpu.SemaphoreType.DMA((3, n_time)),
                pltpu.SemaphoreType.DMA((n_chunks, n_time)),
                pltpu.SemaphoreType.DMA((n_chunks, n_time)),
            ],
            compiler_params=pltpu.CompilerParams(collective_id=0, has_side_effects=True, vmem_limit_bytes=48 * 2**20),
            name="picard",
        )(*(pltpu.with_memory_space_constraint(a, pltpu.HBM) for a in (jnp.swapaxes(x_init, 1, 2), w_in, w_out.T, mod_scale, mod_shift)), step_size)
        return jnp.swapaxes(out, 1, 2)[None]

    return jax.shard_map(local, mesh=mesh, in_specs=(P("data"), P(), P(), P("time"), P("time"), P("time")), out_specs=P("time", "data"), check_vma=False)
```

```python
import functools

import jax
import jax.numpy as jnp
from jax import lax
from jax.experimental import pallas as pl
from jax.experimental.pallas import tpu as pltpu
from jax.sharding import PartitionSpec as P

SWEEPS = 4
TANH_LIN = 0.7978845608028654
TANH_CUB = TANH_LIN * 0.044715
CHUNK = 256
BLOCK = 384
LEAD = 1
LAG = 1
SEND_AFTER = (6, 11, 14)
WAIT_AT = 1


def half_gelu_arg(half):
    square = half * half
    poly = square * (8.0 * TANH_CUB) + 2.0 * TANH_LIN
    gate = jnp.tanh(half * poly)
    return (half * (1.0 + gate)).astype(jnp.bfloat16)


def kernel_body(n_time, x_ref, w_in_ref, w_out_ref, scale_ref, shift_ref, step_ref, out_ref,
                w_in, w_out, step_own, scale_own, shift_own, mods_all, step_all, weights, x_mine, x_half, drifts, x_out,
                local_sem, whole_sem, mod_send, mod_recv, out_send, out_recv):
    me = lax.axis_index("time")
    channels, hidden = w_in.shape
    batch, _, tokens = x_ref.shape
    mine = batch * tokens // n_time
    per_row = tokens // mine
    n_chunks = mine // CHUNK
    n_blocks = hidden // BLOCK
    n_chips = n_time // 2

    def spot(device):
        return lax.div(device, per_row), lax.rem(device, per_row) * mine

    my_row, my_off = spot(me)
    fetches = [
        pltpu.make_async_copy(src, dst, local_sem.at[slot])
        for slot, (src, dst) in enumerate((
            (scale_ref, scale_own), (shift_ref, shift_own), (step_ref, step_own), (w_in_ref, w_in), (w_out_ref, w_out),
            (x_ref.at[my_row, :, pl.ds(pl.multiple_of(my_off, mine), mine)], x_mine)))
    ]
    for fetch in fetches:
        fetch.start()

    chip, core = lax.div(me, 2), lax.rem(me, 2)

    def peer_of(slot):
        return lax.rem(chip + slot // 2, n_chips) * 2 + lax.rem(core + slot % 2, 2)

    def slot_of(step):
        return lax.rem(step // 2 + n_chips - chip, n_chips) * 2 + lax.rem(step % 2 + 2 - core, 2)

    groups = [[1]]
    for dist in range(1, n_chips // 2 + 1):
        ways = (dist,) if 2 * dist == n_chips else (dist, n_chips - dist)
        groups.append([way * 2 + other for way in ways for other in range(2)])
    near_first = [slot for group in groups for slot in group]

    barrier = pltpu.get_barrier_semaphore()
    for slot in reversed(near_first):
        pl.semaphore_signal(barrier, inc=1, device_id={"time": peer_of(slot)}, device_id_type=pl.DeviceIdType.MESH)
    for fetch in fetches:
        fetch.wait()
    mods_all[me] = jnp.concatenate([scale_own[...], shift_own[...]], axis=0)
    step_all[me] = jnp.full(step_all.shape[1:], step_own[0], jnp.float32)

    @pl.when(me == 0)
    def _():
        pltpu.make_async_copy(x_ref, out_ref, whole_sem.at[0]).start()

    def mod_copies(source, target, slot):
        return [
            pltpu.make_async_remote_copy(src_ref=ref.at[source], dst_ref=ref.at[source], send_sem=mod_send.at[kind, slot], recv_sem=mod_recv.at[kind, source],
                                         device_id={"time": target}, device_id_type=pl.DeviceIdType.MESH)
            for kind, ref in enumerate((mods_all, step_all))
        ]

    def prepare(slot):
        mods = mods_all[peer_of(slot)].astype(jnp.float32)
        folded = w_in[...].astype(jnp.float32) * (0.5 * (1.0 + mods[0:1]))
        high = folded.astype(jnp.bfloat16).astype(jnp.float32)
        rest = folded - high
        middle = rest.astype(jnp.bfloat16).astype(jnp.float32)
        low = rest - middle
        first_row = lax.broadcasted_iota(jnp.int32, (channels, hidden), 0) == 0
        bias = jnp.where(first_row, jnp.broadcast_to(0.5 * mods[1:2], (channels, hidden)), 0.0)
        stack = jnp.concatenate([high, middle, low, bias], axis=0)
        weights[slot] = stack.T.astype(jnp.bfloat16)

    ones = jnp.ones((channels, CHUNK), jnp.bfloat16)

    def evaluate(items, extras=None):
        extras = extras or {}
        blocks = [(item, block) for item in range(len(items)) for block in range(n_blocks)]
        stacked, pre, act, drift = {}, {}, {}, {}

        def project(index):
            item, block = blocks[index]
            slot, get_x, _ = items[item]
            if item not in stacked:
                x = get_x()
                stacked[item] = jnp.concatenate([x, x, x, ones], axis=0)
            pre[index] = jnp.dot(weights[slot, block * BLOCK:(block + 1) * BLOCK, :], stacked[item], preferred_element_type=jnp.float32)

        def contract(index):
            item, block = blocks[index]
            part = jnp.dot(w_out[:, block * BLOCK:(block + 1) * BLOCK], act.pop(index), preferred_element_type=jnp.float32)
            drift[item] = part if block == 0 else drift[item] + part
            if block == n_blocks - 1:
                items[item][2](drift.pop(item))

        for index in range(len(blocks) + LEAD + LAG):
            if index < len(blocks):
                for extra in extras.get(index, ()):
                    extra()
                project(index)
            if LEAD <= index < len(blocks) + LEAD:
                act[index - LEAD] = half_gelu_arg(pre.pop(index - LEAD))
            if index >= LEAD + LAG:
                contract(index - LEAD - LAG)

    def columns(chunk):
        return pl.ds(pl.multiple_of(chunk * CHUNK, CHUNK), CHUNK)

    def first_items(slots):
        def item(slot, chunk):
            def put(drift):
                drifts[slot, chunk] = drift
            return slot, lambda: x_mine[:, columns(chunk)].astype(jnp.bfloat16), put
        return [item(slot, chunk) for slot in slots for chunk in range(n_chunks)]

    prepare(0)
    pl.semaphore_wait(barrier, n_time - 1)
    for slot in near_first:
        for copy in mod_copies(me, peer_of(slot), slot):
            copy.start()

    def arrive(slots):
        for slot in slots:
            for copy in mod_copies(peer_of(slot), peer_of(slot), slot):
                copy.wait_recv()

    evaluate(first_items([0]))
    near, middle = len(groups[0] + groups[1]), len(groups[2])
    arrive(near_first[:near])
    for slot in near_first[:near]:
        prepare(slot)
    per_slot = n_chunks * n_blocks
    extras = {WAIT_AT * per_slot: [functools.partial(arrive, near_first[near:near + middle])],
              (WAIT_AT + middle) * per_slot: [functools.partial(arrive, near_first[near + middle:])]}
    for place, slot in enumerate(near_first[near:]):
        extras.setdefault((WAIT_AT + place) * per_slot + 1, []).append(functools.partial(prepare, slot))
    evaluate(first_items(near_first), extras)

    def integrate(chunk):
        last, x = drifts[slot_of(0), chunk], x_mine[:, columns(chunk)]
        for step in range(1, n_time):
            drift = drifts[slot_of(step), chunk]
            x = x + step_all[step - 1] * (0.5 * (last + drift))
            last = drift
            x_half[step] = x.astype(jnp.bfloat16)

    def out_copy(chunk, source, target):
        row, off = spot(source)
        cols = pl.ds(pl.multiple_of(off + chunk * CHUNK, CHUNK), CHUNK)
        return pltpu.make_async_remote_copy(
            src_ref=x_out.at[chunk, target], dst_ref=out_ref.at[row, :, cols], send_sem=out_send.at[chunk, target],
            recv_sem=out_recv.at[chunk, source], device_id={"time": target}, device_id_type=pl.DeviceIdType.MESH)

    def sweep_items(chunk, steps, state):
        def item(step):
            def put(drift):
                state["x"] = state["x"] + step_all[step - 1] * (0.5 * (state["last"] + drift))
                state["last"] = drift
                x_half[step] = state["x"].astype(jnp.bfloat16)
                x_out[chunk, step] = state["x"]
            return slot_of(step), lambda: x_half[step], put
        return [item(step) for step in steps]

    def initial(chunk):
        return {"last": drifts[slot_of(0), chunk], "x": x_mine[:, columns(chunk)]}

    def send(chunk, targets):
        for target in targets:
            @pl.when(me != target)
            def _():
                out_copy(chunk, me, target).start()

    def keep(chunk):
        @pl.when(me != 0)
        def _():
            out_ref[my_row, :, pl.ds(pl.multiple_of(my_off + chunk * CHUNK, CHUNK), CHUNK)] = x_out[chunk, me]

    later = SWEEPS - 1

    def sweep(index, carry):
        chunk = lax.div(index, later)
        evaluate(sweep_items(chunk, range(1, n_time), initial(chunk)))

        @pl.when(jnp.logical_and(lax.rem(index, later) == later - 1, chunk < n_chunks - 1))
        def _():
            send(chunk, range(1, n_time))
            keep(chunk)
            integrate(chunk + 1)
        return carry

    integrate(0)
    lax.fori_loop(0, n_chunks * later - 1, sweep, 0)
    final = n_chunks - 1
    state = initial(final)
    begin = 1
    for end in SEND_AFTER + (n_time,):
        evaluate(sweep_items(final, range(begin, end), state))
        send(final, range(begin, end))
        begin = end
    keep(final)

    for slot in near_first:
        for copy in mod_copies(me, peer_of(slot), slot):
            copy.wait_send()

    @pl.when(me == 0)
    def _():
        pltpu.make_async_copy(x_ref, out_ref, whole_sem.at[0]).wait()

    for chunk in range(n_chunks):
        for target in range(1, n_time):
            @pl.when(me != target)
            def _():
                out_copy(chunk, me, target).wait_send()

    @pl.when(me != 0)
    def _():
        for chunk in range(n_chunks):
            for dist in range(1, n_time):
                out_copy(chunk, lax.rem(me + dist, n_time), me).wait_recv()


def solution(mesh):
    n_time = mesh.shape["time"]

    def local(x_init, w_in, w_out, mod_scale, mod_shift, step_size):
        batch, tokens, channels = x_init.shape
        hidden = w_in.shape[1]
        mine = batch * tokens // n_time
        n_chunks = mine // CHUNK
        out = pl.pallas_call(
            functools.partial(kernel_body, n_time),
            out_shape=jax.ShapeDtypeStruct((batch, channels, tokens), jnp.float32),
            in_specs=[pl.BlockSpec(memory_space=pltpu.HBM)] * 6,
            out_specs=pl.BlockSpec(memory_space=pltpu.VMEM),
            scratch_shapes=[
                pltpu.VMEM((channels, hidden), jnp.bfloat16),
                pltpu.VMEM((channels, hidden), jnp.bfloat16),
                pltpu.SMEM((1,), jnp.float32),
                pltpu.VMEM((1, hidden), jnp.bfloat16),
                pltpu.VMEM((1, hidden), jnp.bfloat16),
                pltpu.VMEM((n_time, 2, hidden), jnp.bfloat16),
                pltpu.VMEM((n_time, 1, CHUNK), jnp.float32),
                pltpu.VMEM((n_time, hidden, 4 * channels), jnp.bfloat16),
                pltpu.VMEM((channels, mine), jnp.float32),
                pltpu.VMEM((n_time, channels, CHUNK), jnp.bfloat16),
                pltpu.VMEM((n_time, n_chunks, channels, CHUNK), jnp.float32),
                pltpu.VMEM((n_chunks, n_time, channels, CHUNK), jnp.float32),
                pltpu.SemaphoreType.DMA((6,)),
                pltpu.SemaphoreType.DMA((1,)),
                pltpu.SemaphoreType.DMA((2, n_time)),
                pltpu.SemaphoreType.DMA((2, n_time)),
                pltpu.SemaphoreType.DMA((n_chunks, n_time)),
                pltpu.SemaphoreType.DMA((n_chunks, n_time)),
            ],
            compiler_params=pltpu.CompilerParams(collective_id=0, has_side_effects=True, vmem_limit_bytes=48 * 2**20),
            name="picard",
        )(*(pltpu.with_memory_space_constraint(a, pltpu.HBM) for a in (jnp.swapaxes(x_init, 1, 2), w_in, w_out.T, mod_scale, mod_shift)), step_size)
        return jnp.swapaxes(out, 1, 2)[None]

    return jax.shard_map(local, mesh=mesh, in_specs=(P("data"), P(), P(), P("time"), P("time"), P("time")), out_specs=P("time", "data"), check_vma=False)
```

```python
import functools

import jax
import jax.numpy as jnp
from jax import lax
from jax.experimental import pallas as pl
from jax.experimental.pallas import tpu as pltpu
from jax.sharding import PartitionSpec as P

SWEEPS = 4
TANH_LIN = 0.7978845608028654
TANH_CUB = TANH_LIN * 0.044715
CHUNK = 256
BLOCK = 384
LEAD = 1
LAG = 1
WAIT_AT = 1
SEND_AFTER = (5, 9, 12, 14)


def half_gelu_arg(half):
    square = half * half
    poly = square * (8.0 * TANH_CUB) + 2.0 * TANH_LIN
    gate = jnp.tanh(half * poly)
    return (half * (1.0 + gate)).astype(jnp.bfloat16)


def kernel_body(n_time, x_ref, w_in_ref, w_out_ref, scale_ref, shift_ref, step_ref, out_ref,
                w_in, w_out, step_own, scale_own, shift_own, mods_all, step_all, weights, x_mine, x_half, drifts, x_out, landed,
                local_sem, whole_sem, mod_send, mod_recv, out_send, out_recv):
    me = lax.axis_index("time")
    channels, hidden = w_in.shape
    batch, _, tokens = x_ref.shape
    mine = batch * tokens // n_time
    per_row = tokens // mine
    n_chunks = mine // CHUNK
    n_blocks = hidden // BLOCK
    n_chips = n_time // 2

    def spot(device):
        return lax.div(device, per_row), lax.rem(device, per_row) * mine

    my_row, my_off = spot(me)
    fetches = [
        pltpu.make_async_copy(src, dst, local_sem.at[slot])
        for slot, (src, dst) in enumerate((
            (scale_ref, scale_own), (shift_ref, shift_own), (step_ref, step_own), (w_in_ref, w_in), (w_out_ref, w_out),
            (x_ref.at[my_row, :, pl.ds(pl.multiple_of(my_off, mine), mine)], x_mine)))
    ]
    for fetch in fetches:
        fetch.start()

    chip, core = lax.div(me, 2), lax.rem(me, 2)

    def peer_of(slot):
        return lax.rem(chip + slot // 2, n_chips) * 2 + lax.rem(core + slot % 2, 2)

    def slot_of(step):
        return lax.rem(step // 2 + n_chips - chip, n_chips) * 2 + lax.rem(step % 2 + 2 - core, 2)

    groups = [[1]]
    for dist in range(1, n_chips // 2 + 1):
        ways = (dist,) if 2 * dist == n_chips else (dist, n_chips - dist)
        groups.append([way * 2 + other for way in ways for other in range(2)])
    near_first = [slot for group in groups for slot in group]

    barrier = pltpu.get_barrier_semaphore()
    for slot in reversed(near_first):
        pl.semaphore_signal(barrier, inc=1, device_id={"time": peer_of(slot)}, device_id_type=pl.DeviceIdType.MESH)
    for fetch in fetches:
        fetch.wait()
    mods_all[me] = jnp.concatenate([scale_own[...], shift_own[...]], axis=0)
    step_all[me] = jnp.full(step_all.shape[1:], step_own[0], jnp.float32)

    @pl.when(me == 0)
    def _():
        pltpu.make_async_copy(x_ref, landed.at[pl.ds(0, batch)], whole_sem.at[0]).start()

    def mod_copies(source, target, slot):
        return [
            pltpu.make_async_remote_copy(src_ref=ref.at[source], dst_ref=ref.at[source], send_sem=mod_send.at[kind, slot], recv_sem=mod_recv.at[kind, source],
                                         device_id={"time": target}, device_id_type=pl.DeviceIdType.MESH)
            for kind, ref in enumerate((mods_all, step_all))
        ]

    def prepare(slot):
        mods = mods_all[peer_of(slot)].astype(jnp.float32)
        folded = w_in[...].astype(jnp.float32) * (0.5 * (1.0 + mods[0:1]))
        high = folded.astype(jnp.bfloat16).astype(jnp.float32)
        rest = folded - high
        middle = rest.astype(jnp.bfloat16).astype(jnp.float32)
        low = rest - middle
        first_row = lax.broadcasted_iota(jnp.int32, (channels, hidden), 0) == 0
        bias = jnp.where(first_row, jnp.broadcast_to(0.5 * mods[1:2], (channels, hidden)), 0.0)
        stack = jnp.concatenate([high, middle, low, bias], axis=0)
        weights[slot] = stack.T.astype(jnp.bfloat16)

    ones = jnp.ones((channels, CHUNK), jnp.bfloat16)

    def evaluate(items, extras=None):
        extras = extras or {}
        blocks = [(item, block) for item in range(len(items)) for block in range(n_blocks)]
        stacked, pre, act, drift = {}, {}, {}, {}

        def project(index):
            item, block = blocks[index]
            slot, get_x, _ = items[item]
            if item not in stacked:
                x = get_x()
                stacked[item] = jnp.concatenate([x, x, x, ones], axis=0)
            pre[index] = jnp.dot(weights[slot, block * BLOCK:(block + 1) * BLOCK, :], stacked[item], preferred_element_type=jnp.float32)

        def contract(index):
            item, block = blocks[index]
            part = jnp.dot(w_out[:, block * BLOCK:(block + 1) * BLOCK], act.pop(index), preferred_element_type=jnp.float32)
            drift[item] = part if block == 0 else drift[item] + part
            if block == n_blocks - 1:
                items[item][2](drift.pop(item))

        for index in range(len(blocks) + LEAD + LAG + 1):
            for extra in extras.get(index, ()):
                extra()
            if index < len(blocks):
                project(index)
            if LEAD <= index < len(blocks) + LEAD:
                act[index - LEAD] = half_gelu_arg(pre.pop(index - LEAD))
            if LEAD + LAG <= index < len(blocks) + LEAD + LAG:
                contract(index - LEAD - LAG)

    def columns(chunk):
        return pl.ds(pl.multiple_of(chunk * CHUNK, CHUNK), CHUNK)

    def first_items(slots):
        def item(slot, chunk):
            def put(drift):
                drifts[slot, chunk] = drift
            return slot, lambda: x_mine[:, columns(chunk)].astype(jnp.bfloat16), put
        return [item(slot, chunk) for slot in slots for chunk in range(n_chunks)]

    prepare(0)
    pl.semaphore_wait(barrier, n_time - 1)
    for slot in near_first:
        for copy in mod_copies(me, peer_of(slot), slot):
            copy.start()

    def arrive(slots):
        for slot in slots:
            for copy in mod_copies(peer_of(slot), peer_of(slot), slot):
                copy.wait_recv()

    evaluate(first_items([0]))
    near, middle = len(groups[0] + groups[1]), len(groups[2])
    arrive(near_first[:near])
    for slot in near_first[:near]:
        prepare(slot)
    per_slot = n_chunks * n_blocks
    extras = {WAIT_AT * per_slot: [functools.partial(arrive, near_first[near:near + middle])],
              (WAIT_AT + middle) * per_slot: [functools.partial(arrive, near_first[near + middle:])]}
    for place, slot in enumerate(near_first[near:]):
        extras.setdefault((WAIT_AT + place) * per_slot + 1, []).append(functools.partial(prepare, slot))
    evaluate(first_items(near_first), extras)

    def integrate(chunk):
        last, x = drifts[slot_of(0), chunk], x_mine[:, columns(chunk)]
        for step in range(1, n_time):
            drift = drifts[slot_of(step), chunk]
            x = x + step_all[step - 1] * (0.5 * (last + drift))
            last = drift
            x_half[step] = x.astype(jnp.bfloat16)

    def out_copy(chunk, source, target):
        row, off = spot(source)
        cols = pl.ds(pl.multiple_of(off + chunk * CHUNK, CHUNK), CHUNK)
        own = source == target
        return pltpu.make_async_remote_copy(
            src_ref=x_out.at[chunk, target], dst_ref=landed.at[jnp.where(own, batch, row), :, cols], send_sem=out_send.at[chunk, target],
            recv_sem=out_recv.at[chunk, jnp.where(own, n_time, source)], device_id={"time": jnp.where(own, target + 1 - 2 * lax.rem(target, 2), target)},
            device_id_type=pl.DeviceIdType.MESH)

    def sweep_items(chunk, steps, state):
        def item(step):
            def put(drift):
                state["x"] = state["x"] + step_all[step - 1] * (0.5 * (state["last"] + drift))
                state["last"] = drift
                x_half[step] = state["x"].astype(jnp.bfloat16)
                x_out[chunk, step] = state["x"]
            return slot_of(step), lambda: x_half[step], put
        return [item(step) for step in steps]

    def initial(chunk):
        return {"last": drifts[slot_of(0), chunk], "x": x_mine[:, columns(chunk)]}

    def send(chunk, target):
        out_copy(chunk, me, target).start()

    def keep(chunk):
        @pl.when(me != 0)
        def _():
            landed[my_row, :, pl.ds(pl.multiple_of(my_off + chunk * CHUNK, CHUNK), CHUNK)] = x_out[chunk, me]

    later = SWEEPS - 1

    def sweep(index, carry):
        chunk = lax.div(index, later)
        evaluate(sweep_items(chunk, range(1, n_time), initial(chunk)))

        @pl.when(jnp.logical_and(lax.rem(index, later) == later - 1, chunk < n_chunks - 1))
        def _():
            for target in range(1, n_time):
                send(chunk, target)
            keep(chunk)
            integrate(chunk + 1)
        return carry

    integrate(0)
    lax.fori_loop(0, n_chunks * later - 1, sweep, 0)
    final = n_chunks - 1
    sends, begin = {}, 1
    for end in SEND_AFTER + (n_time - 1,):
        sends[end * n_blocks + LEAD + LAG] = [functools.partial(send, final, target) for target in range(begin, end + 1)]
        begin = end + 1
    evaluate(sweep_items(final, range(1, n_time), initial(final)), sends)
    keep(final)

    for slot in near_first:
        for copy in mod_copies(me, peer_of(slot), slot):
            copy.wait_send()

    @pl.when(me == 0)
    def _():
        pltpu.make_async_copy(x_ref, landed.at[pl.ds(0, batch)], whole_sem.at[0]).wait()

    for chunk in range(n_chunks):
        for target in range(1, n_time):
            out_copy(chunk, me, target).wait_send()

    @pl.when(me != 1)
    def _():
        for chunk in range(n_chunks):
            pair = me + 1 - 2 * lax.rem(me, 2)
            out_copy(chunk, pair, pair).wait_recv()

    @pl.when(me != 0)
    def _():
        for chunk in range(n_chunks):
            for dist in range(1, n_time):
                out_copy(chunk, lax.rem(me + dist, n_time), me).wait_recv()

    out_ref[...] = landed[0:batch]


def solution(mesh):
    n_time = mesh.shape["time"]

    def local(x_init, w_in, w_out, mod_scale, mod_shift, step_size):
        batch, tokens, channels = x_init.shape
        hidden = w_in.shape[1]
        mine = batch * tokens // n_time
        n_chunks = mine // CHUNK
        out = pl.pallas_call(
            functools.partial(kernel_body, n_time),
            out_shape=jax.ShapeDtypeStruct((batch, channels, tokens), jnp.float32),
            in_specs=[pl.BlockSpec(memory_space=pltpu.HBM)] * 6,
            out_specs=pl.BlockSpec(memory_space=pltpu.VMEM),
            scratch_shapes=[
                pltpu.VMEM((channels, hidden), jnp.bfloat16),
                pltpu.VMEM((channels, hidden), jnp.bfloat16),
                pltpu.SMEM((1,), jnp.float32),
                pltpu.VMEM((1, hidden), jnp.bfloat16),
                pltpu.VMEM((1, hidden), jnp.bfloat16),
                pltpu.VMEM((n_time, 2, hidden), jnp.bfloat16),
                pltpu.VMEM((n_time, 1, CHUNK), jnp.float32),
                pltpu.VMEM((n_time, hidden, 4 * channels), jnp.bfloat16),
                pltpu.VMEM((channels, mine), jnp.float32),
                pltpu.VMEM((n_time, channels, CHUNK), jnp.bfloat16),
                pltpu.VMEM((n_time, n_chunks, channels, CHUNK), jnp.float32),
                pltpu.VMEM((n_chunks, n_time, channels, CHUNK), jnp.float32),
                pltpu.VMEM((batch + 1, channels, tokens), jnp.float32),
                pltpu.SemaphoreType.DMA((6,)),
                pltpu.SemaphoreType.DMA((1,)),
                pltpu.SemaphoreType.DMA((2, n_time)),
                pltpu.SemaphoreType.DMA((2, n_time)),
                pltpu.SemaphoreType.DMA((n_chunks, n_time)),
                pltpu.SemaphoreType.DMA((n_chunks, n_time + 1)),
            ],
            compiler_params=pltpu.CompilerParams(collective_id=0, has_side_effects=True, vmem_limit_bytes=48 * 2**20),
            name="picard",
        )(*(pltpu.with_memory_space_constraint(a, pltpu.HBM) for a in (jnp.swapaxes(x_init, 1, 2), w_in, w_out.T, mod_scale, mod_shift)), step_size)
        return jnp.swapaxes(out, 1, 2)[None]

    return jax.shard_map(local, mesh=mesh, in_specs=(P("data"), P(), P(), P("time"), P("time"), P("time")), out_specs=P("time", "data"), check_vma=False)
```

```python
import functools

import jax
import jax.numpy as jnp
from jax import lax
from jax.experimental import pallas as pl
from jax.experimental.pallas import tpu as pltpu
from jax.sharding import PartitionSpec as P

SWEEPS = 4
TANH_LIN = 0.7978845608028654
TANH_CUB = TANH_LIN * 0.044715
CHUNK = 256
BLOCK = 384
LEAD = 1
LAG = 1
SEND_AFTER = (6, 11, 14)
LENT = 9
EARLY = 5
AHEAD = 2


def half_gelu_arg(half):
    square = half * half
    poly = square * (8.0 * TANH_CUB) + 2.0 * TANH_LIN
    gate = jnp.tanh(half * poly)
    return (half * (1.0 + gate)).astype(jnp.bfloat16)


def kernel_body(n_time, x_ref, w_in_ref, w_out_ref, scale_ref, shift_ref, step_ref, out_ref,
                w_in, w_out, step_own, scale_own, shift_own, mods_all, step_all, weights, x_mine, x_whole, x_half, drifts, drift_out, x_out,
                local_sem, whole_sem, mod_send, mod_recv, drift_send, drift_recv, out_send, out_recv):
    me = lax.axis_index("time")
    channels, hidden = w_in.shape
    batch, _, tokens = x_ref.shape
    mine = batch * tokens // n_time
    per_row = tokens // mine
    n_chunks = mine // CHUNK
    n_blocks = hidden // BLOCK
    n_chips = n_time // 2

    def spot(device):
        return lax.div(device, per_row), lax.rem(device, per_row) * mine

    my_row, my_off = spot(me)
    fetches = [
        pltpu.make_async_copy(src, dst, local_sem.at[slot])
        for slot, (src, dst) in enumerate((
            (scale_ref, scale_own), (shift_ref, shift_own), (step_ref, step_own), (w_in_ref, w_in), (w_out_ref, w_out),
            (x_ref.at[my_row, :, pl.ds(pl.multiple_of(my_off, mine), mine)], x_mine), (x_ref, x_whole)))
    ]
    for fetch in fetches:
        fetch.start()

    chip, core = lax.div(me, 2), lax.rem(me, 2)

    def peer_of(slot):
        return lax.rem(chip + slot // 2, n_chips) * 2 + lax.rem(core + slot % 2, 2)

    def slot_of(step):
        return lax.rem(step // 2 + n_chips - chip, n_chips) * 2 + lax.rem(step % 2 + 2 - core, 2)

    groups = [[1]]
    for dist in range(1, n_chips // 2 + 1):
        ways = (dist,) if 2 * dist == n_chips else (dist, n_chips - dist)
        groups.append([way * 2 + other for way in ways for other in range(2)])
    near_first = [slot for group in groups for slot in group]

    barrier = pltpu.get_barrier_semaphore()
    for slot in reversed(near_first):
        pl.semaphore_signal(barrier, inc=1, device_id={"time": peer_of(slot)}, device_id_type=pl.DeviceIdType.MESH)
    for fetch in fetches:
        fetch.wait()
    mods_all[me] = jnp.concatenate([scale_own[...], shift_own[...]], axis=0)
    step_all[me] = jnp.full(step_all.shape[1:], step_own[0], jnp.float32)

    @pl.when(me == 0)
    def _():
        pltpu.make_async_copy(x_ref, out_ref, whole_sem.at[0]).start()

    def mod_copies(source, target, slot):
        return [
            pltpu.make_async_remote_copy(src_ref=ref.at[source], dst_ref=ref.at[source], send_sem=mod_send.at[kind, slot], recv_sem=mod_recv.at[kind, source],
                                         device_id={"time": target}, device_id_type=pl.DeviceIdType.MESH)
            for kind, ref in enumerate((mods_all, step_all))
        ]

    def prepare(slot):
        mods = mods_all[peer_of(slot)].astype(jnp.float32)
        folded = w_in[...].astype(jnp.float32) * (0.5 * (1.0 + mods[0:1]))
        high = folded.astype(jnp.bfloat16).astype(jnp.float32)
        rest = folded - high
        middle = rest.astype(jnp.bfloat16).astype(jnp.float32)
        low = rest - middle
        first_row = lax.broadcasted_iota(jnp.int32, (channels, hidden), 0) == 0
        bias = jnp.where(first_row, jnp.broadcast_to(0.5 * mods[1:2], (channels, hidden)), 0.0)
        stack = jnp.concatenate([high, middle, low, bias], axis=0)
        weights[slot] = stack.T.astype(jnp.bfloat16)

    ones = jnp.ones((channels, CHUNK), jnp.bfloat16)

    def evaluate(items, extras=None):
        extras = extras or {}
        blocks = [(item, block) for item in range(len(items)) for block in range(n_blocks)]
        stacked, pre, act, drift = {}, {}, {}, {}

        def project(index):
            item, block = blocks[index]
            slot, get_x, _ = items[item]
            if item not in stacked:
                x = get_x()
                stacked[item] = jnp.concatenate([x, x, x, ones], axis=0)
            pre[index] = jnp.dot(weights[slot, block * BLOCK:(block + 1) * BLOCK, :], stacked[item], preferred_element_type=jnp.float32)

        def contract(index):
            item, block = blocks[index]
            part = jnp.dot(w_out[:, block * BLOCK:(block + 1) * BLOCK], act.pop(index), preferred_element_type=jnp.float32)
            drift[item] = part if block == 0 else drift[item] + part
            if block == n_blocks - 1:
                items[item][2](drift.pop(item))

        for index in range(len(blocks) + LEAD + LAG):
            if index < len(blocks):
                for extra in extras.get(index, ()):
                    extra()
                project(index)
            if LEAD <= index < len(blocks) + LEAD:
                act[index - LEAD] = half_gelu_arg(pre.pop(index - LEAD))
            if index >= LEAD + LAG:
                contract(index - LEAD - LAG)

    def columns(chunk):
        return pl.ds(pl.multiple_of(chunk * CHUNK, CHUNK), CHUNK)

    def first_items(slots):
        def item(slot, chunk):
            def put(drift):
                drifts[slot, chunk] = drift
            return slot, lambda: x_mine[:, columns(chunk)].astype(jnp.bfloat16), put
        return [item(slot, chunk) for slot in slots for chunk in range(n_chunks)]

    def lent_items(places):
        def item(place, chunk):
            row, off = spot(peer_of(near_first[place]))
            def get():
                return x_whole[row, :, pl.ds(pl.multiple_of(off + chunk * CHUNK, CHUNK), CHUNK)].astype(jnp.bfloat16)
            def put(drift):
                drift_out[place, chunk] = drift
            return 0, get, put
        return [item(place, chunk) for place in places for chunk in range(n_chunks)]

    def drift_copy(place):
        slot = near_first[place]
        back = (n_chips - slot // 2) % n_chips * 2 + slot % 2
        return pltpu.make_async_remote_copy(
            src_ref=drift_out.at[place], dst_ref=drifts.at[back], send_sem=drift_send.at[place], recv_sem=drift_recv.at[back],
            device_id={"time": peer_of(slot)}, device_id_type=pl.DeviceIdType.MESH)

    def drift_arrival(slot):
        return pltpu.make_async_remote_copy(
            src_ref=drift_out.at[0], dst_ref=drifts.at[slot], send_sem=drift_send.at[0], recv_sem=drift_recv.at[slot],
            device_id={"time": peer_of(slot)}, device_id_type=pl.DeviceIdType.MESH)

    def arrive(slots):
        for slot in slots:
            for copy in mod_copies(peer_of(slot), peer_of(slot), slot):
                copy.wait_recv()

    prepare(0)
    evaluate(first_items([0]) + lent_items(range(EARLY)))
    pl.semaphore_wait(barrier, n_time - 1)
    far, near = near_first[LENT:], near_first[:LENT]
    for slot in far + near:
        for copy in mod_copies(me, peer_of(slot), slot):
            copy.start()
    for place in range(EARLY):
        drift_copy(place).start()
    evaluate(lent_items(range(EARLY, LENT)))
    for place in range(EARLY, LENT):
        drift_copy(place).start()
    per_slot = n_chunks * n_blocks
    arrive(far[:AHEAD])
    for slot in far[:AHEAD]:
        prepare(slot)
    extras = {1: [functools.partial(arrive, far[AHEAD:])], (len(far) - AHEAD) * per_slot: [functools.partial(arrive, near)]}
    for place, slot in enumerate(far[AHEAD:]):
        extras.setdefault(place * per_slot + 2, []).append(functools.partial(prepare, slot))
    rest = AHEAD * per_slot
    for place, slot in enumerate(near):
        extras.setdefault(min((len(far) - AHEAD) * per_slot + 1 + place * rest // len(near), len(far) * per_slot - 1), []).append(functools.partial(prepare, slot))
    evaluate(first_items(far), extras)
    for slot in near:
        drift_arrival(slot).wait_recv()

    def integrate(chunk):
        last, x = drifts[slot_of(0), chunk], x_mine[:, columns(chunk)]
        for step in range(1, n_time):
            drift = drifts[slot_of(step), chunk]
            x = x + step_all[step - 1] * (0.5 * (last + drift))
            last = drift
            x_half[step] = x.astype(jnp.bfloat16)

    def out_copy(chunk, source, target):
        row, off = spot(source)
        cols = pl.ds(pl.multiple_of(off + chunk * CHUNK, CHUNK), CHUNK)
        return pltpu.make_async_remote_copy(
            src_ref=x_out.at[chunk, target], dst_ref=out_ref.at[row, :, cols], send_sem=out_send.at[chunk, target],
            recv_sem=out_recv.at[chunk, source], device_id={"time": target}, device_id_type=pl.DeviceIdType.MESH)

    def sweep_items(chunk, steps, state):
        def item(step):
            def put(drift):
                state["x"] = state["x"] + step_all[step - 1] * (0.5 * (state["last"] + drift))
                state["last"] = drift
                x_half[step] = state["x"].astype(jnp.bfloat16)
                x_out[chunk, step] = state["x"]
            return slot_of(step), lambda: x_half[step], put
        return [item(step) for step in steps]

    def initial(chunk):
        return {"last": drifts[slot_of(0), chunk], "x": x_mine[:, columns(chunk)]}

    def send(chunk, targets):
        for target in targets:
            @pl.when(me != target)
            def _():
                out_copy(chunk, me, target).start()

    def keep(chunk):
        @pl.when(me != 0)
        def _():
            out_ref[my_row, :, pl.ds(pl.multiple_of(my_off + chunk * CHUNK, CHUNK), CHUNK)] = x_out[chunk, me]

    later = SWEEPS - 1

    def sweep(index, carry):
        chunk = lax.div(index, later)
        evaluate(sweep_items(chunk, range(1, n_time), initial(chunk)))

        @pl.when(jnp.logical_and(lax.rem(index, later) == later - 1, chunk < n_chunks - 1))
        def _():
            send(chunk, range(1, n_time))
            keep(chunk)
            integrate(chunk + 1)
        return carry

    integrate(0)
    lax.fori_loop(0, n_chunks * later - 1, sweep, 0)
    final = n_chunks - 1
    state = initial(final)
    begin = 1
    for end in SEND_AFTER + (n_time,):
        evaluate(sweep_items(final, range(begin, end), state))
        send(final, range(begin, end))
        begin = end
    keep(final)

    for slot in near_first:
        for copy in mod_copies(me, peer_of(slot), slot):
            copy.wait_send()
    for place in range(LENT):
        drift_copy(place).wait_send()

    @pl.when(me == 0)
    def _():
        pltpu.make_async_copy(x_ref, out_ref, whole_sem.at[0]).wait()

    for chunk in range(n_chunks):
        for target in range(1, n_time):
            @pl.when(me != target)
            def _():
                out_copy(chunk, me, target).wait_send()

    @pl.when(me != 0)
    def _():
        for chunk in range(n_chunks):
            for dist in range(1, n_time):
                out_copy(chunk, lax.rem(me + dist, n_time), me).wait_recv()


def solution(mesh):
    n_time = mesh.shape["time"]

    def local(x_init, w_in, w_out, mod_scale, mod_shift, step_size):
        batch, tokens, channels = x_init.shape
        hidden = w_in.shape[1]
        mine = batch * tokens // n_time
        n_chunks = mine // CHUNK
        out = pl.pallas_call(
            functools.partial(kernel_body, n_time),
            out_shape=jax.ShapeDtypeStruct((batch, channels, tokens), jnp.float32),
            in_specs=[pl.BlockSpec(memory_space=pltpu.HBM)] * 6,
            out_specs=pl.BlockSpec(memory_space=pltpu.VMEM),
            scratch_shapes=[
                pltpu.VMEM((channels, hidden), jnp.bfloat16),
                pltpu.VMEM((channels, hidden), jnp.bfloat16),
                pltpu.SMEM((1,), jnp.float32),
                pltpu.VMEM((1, hidden), jnp.bfloat16),
                pltpu.VMEM((1, hidden), jnp.bfloat16),
                pltpu.VMEM((n_time, 2, hidden), jnp.bfloat16),
                pltpu.VMEM((n_time, 1, CHUNK), jnp.float32),
                pltpu.VMEM((n_time, hidden, 4 * channels), jnp.bfloat16),
                pltpu.VMEM((channels, mine), jnp.float32),
                pltpu.VMEM((batch, channels, tokens), jnp.float32),
                pltpu.VMEM((n_time, channels, CHUNK), jnp.bfloat16),
                pltpu.VMEM((n_time, n_chunks, channels, CHUNK), jnp.float32),
                pltpu.VMEM((LENT, n_chunks, channels, CHUNK), jnp.float32),
                pltpu.VMEM((n_chunks, n_time, channels, CHUNK), jnp.float32),
                pltpu.SemaphoreType.DMA((7,)),
                pltpu.SemaphoreType.DMA((1,)),
                pltpu.SemaphoreType.DMA((2, n_time)),
                pltpu.SemaphoreType.DMA((2, n_time)),
                pltpu.SemaphoreType.DMA((LENT,)),
                pltpu.SemaphoreType.DMA((n_time,)),
                pltpu.SemaphoreType.DMA((n_chunks, n_time)),
                pltpu.SemaphoreType.DMA((n_chunks, n_time)),
            ],
            compiler_params=pltpu.CompilerParams(collective_id=0, has_side_effects=True, vmem_limit_bytes=48 * 2**20),
            name="picard",
        )(*(pltpu.with_memory_space_constraint(a, pltpu.HBM) for a in (jnp.swapaxes(x_init, 1, 2), w_in, w_out.T, mod_scale, mod_shift)), step_size)
        return jnp.swapaxes(out, 1, 2)[None]

    return jax.shard_map(local, mesh=mesh, in_specs=(P("data"), P(), P(), P("time"), P("time"), P("time")), out_specs=P("time", "data"), check_vma=False)
```

```python
import functools

import jax
import jax.numpy as jnp
from jax import lax
from jax.experimental import pallas as pl
from jax.experimental.pallas import tpu as pltpu
from jax.sharding import PartitionSpec as P

SWEEPS = 4
TANH_LIN = 0.7978845608028654
TANH_CUB = TANH_LIN * 0.044715
CHUNK = 256
BLOCK = 384
LEAD = 1
LAG = 1
SEND_AFTER = (6, 11, 14)
LENT = 9
EARLY = 2
AHEAD = 2


def half_gelu_arg(half):
    square = half * half
    poly = square * (8.0 * TANH_CUB) + 2.0 * TANH_LIN
    gate = jnp.tanh(half * poly)
    return (half * (1.0 + gate)).astype(jnp.bfloat16)


def kernel_body(n_time, x_ref, w_in_ref, w_out_ref, scale_ref, shift_ref, step_ref, out_ref,
                w_in, w_out, step_own, scale_own, shift_own, mods_all, step_all, weights, x_mine, x_whole, x_half, drifts, drift_out, x_out,
                local_sem, whole_sem, mod_send, mod_recv, drift_send, drift_recv, out_send, out_recv):
    me = lax.axis_index("time")
    channels, hidden = w_in.shape
    batch, _, tokens = x_ref.shape
    mine = batch * tokens // n_time
    per_row = tokens // mine
    n_chunks = mine // CHUNK
    n_blocks = hidden // BLOCK
    n_chips = n_time // 2

    def spot(device):
        return lax.div(device, per_row), lax.rem(device, per_row) * mine

    my_row, my_off = spot(me)
    fetches = [
        pltpu.make_async_copy(src, dst, local_sem.at[slot])
        for slot, (src, dst) in enumerate((
            (scale_ref, scale_own), (shift_ref, shift_own), (step_ref, step_own), (w_in_ref, w_in), (w_out_ref, w_out),
            (x_ref.at[my_row, :, pl.ds(pl.multiple_of(my_off, mine), mine)], x_mine), (x_ref, x_whole)))
    ]
    for fetch in fetches:
        fetch.start()

    chip, core = lax.div(me, 2), lax.rem(me, 2)

    def peer_of(slot):
        return lax.rem(chip + slot // 2, n_chips) * 2 + lax.rem(core + slot % 2, 2)

    def slot_of(step):
        return lax.rem(step // 2 + n_chips - chip, n_chips) * 2 + lax.rem(step % 2 + 2 - core, 2)

    groups = [[1]]
    for dist in range(1, n_chips // 2 + 1):
        ways = (dist,) if 2 * dist == n_chips else (dist, n_chips - dist)
        groups.append([way * 2 + other for way in ways for other in range(2)])
    near_first = [slot for group in groups for slot in group]

    barrier = pltpu.get_barrier_semaphore()
    for slot in reversed(near_first):
        pl.semaphore_signal(barrier, inc=1, device_id={"time": peer_of(slot)}, device_id_type=pl.DeviceIdType.MESH)
    for fetch in fetches:
        fetch.wait()
    mods_all[me] = jnp.concatenate([scale_own[...], shift_own[...]], axis=0)
    step_all[me] = jnp.full(step_all.shape[1:], step_own[0], jnp.float32)

    @pl.when(me == 0)
    def _():
        pltpu.make_async_copy(x_ref, out_ref, whole_sem.at[0]).start()

    def mod_copies(source, target, slot):
        return [
            pltpu.make_async_remote_copy(src_ref=ref.at[source], dst_ref=ref.at[source], send_sem=mod_send.at[kind, slot], recv_sem=mod_recv.at[kind, source],
                                         device_id={"time": target}, device_id_type=pl.DeviceIdType.MESH)
            for kind, ref in enumerate((mods_all, step_all))
        ]

    def prepare(slot):
        mods = mods_all[peer_of(slot)].astype(jnp.float32)
        folded = w_in[...].astype(jnp.float32) * (0.5 * (1.0 + mods[0:1]))
        high = folded.astype(jnp.bfloat16).astype(jnp.float32)
        rest = folded - high
        middle = rest.astype(jnp.bfloat16).astype(jnp.float32)
        low = rest - middle
        first_row = lax.broadcasted_iota(jnp.int32, (channels, hidden), 0) == 0
        bias = jnp.where(first_row, jnp.broadcast_to(0.5 * mods[1:2], (channels, hidden)), 0.0)
        stack = jnp.concatenate([high, middle, low, bias], axis=0)
        weights[slot] = stack.T.astype(jnp.bfloat16)

    ones = jnp.ones((channels, CHUNK), jnp.bfloat16)

    def evaluate(items, extras=None):
        extras = extras or {}
        blocks = [(item, block) for item in range(len(items)) for block in range(n_blocks)]
        stacked, pre, act, drift = {}, {}, {}, {}

        def project(index):
            item, block = blocks[index]
            slot, get_x, _ = items[item]
            if item not in stacked:
                x = get_x()
                stacked[item] = jnp.concatenate([x, x, x, ones], axis=0)
            pre[index] = jnp.dot(weights[slot, block * BLOCK:(block + 1) * BLOCK, :], stacked[item], preferred_element_type=jnp.float32)

        def contract(index):
            item, block = blocks[index]
            part = jnp.dot(w_out[:, block * BLOCK:(block + 1) * BLOCK], act.pop(index), preferred_element_type=jnp.float32)
            drift[item] = part if block == 0 else drift[item] + part
            if block == n_blocks - 1:
                items[item][2](drift.pop(item))

        for index in range(len(blocks) + LEAD + LAG):
            if index < len(blocks):
                for extra in extras.get(index, ()):
                    extra()
                project(index)
            if LEAD <= index < len(blocks) + LEAD:
                act[index - LEAD] = half_gelu_arg(pre.pop(index - LEAD))
            if index >= LEAD + LAG:
                contract(index - LEAD - LAG)

    def columns(chunk):
        return pl.ds(pl.multiple_of(chunk * CHUNK, CHUNK), CHUNK)

    def first_items(slots):
        def item(slot, chunk):
            def put(drift):
                drifts[slot, chunk] = drift
            return slot, lambda: x_mine[:, columns(chunk)].astype(jnp.bfloat16), put
        return [item(slot, chunk) for slot in slots for chunk in range(n_chunks)]

    def lent_items(places):
        def item(place, chunk):
            row, off = spot(peer_of(near_first[place]))
            def get():
                return x_whole[row, :, pl.ds(pl.multiple_of(off + chunk * CHUNK, CHUNK), CHUNK)].astype(jnp.bfloat16)
            def put(drift):
                drift_out[place, chunk] = drift
            return 0, get, put
        return [item(place, chunk) for place in places for chunk in range(n_chunks)]

    def drift_copy(place):
        slot = near_first[place]
        back = (n_chips - slot // 2) % n_chips * 2 + slot % 2
        return pltpu.make_async_remote_copy(
            src_ref=drift_out.at[place], dst_ref=drifts.at[back], send_sem=drift_send.at[place], recv_sem=drift_recv.at[back],
            device_id={"time": peer_of(slot)}, device_id_type=pl.DeviceIdType.MESH)

    def drift_arrival(slot):
        return pltpu.make_async_remote_copy(
            src_ref=drift_out.at[0], dst_ref=drifts.at[slot], send_sem=drift_send.at[0], recv_sem=drift_recv.at[slot],
            device_id={"time": peer_of(slot)}, device_id_type=pl.DeviceIdType.MESH)

    def arrive(slots):
        for slot in slots:
            for copy in mod_copies(peer_of(slot), peer_of(slot), slot):
                copy.wait_recv()

    prepare(0)
    evaluate(first_items([0]) + lent_items(range(EARLY)))
    pl.semaphore_wait(barrier, n_time - 1)
    far, near = near_first[LENT:], near_first[:LENT]
    for slot in far + near:
        for copy in mod_copies(me, peer_of(slot), slot):
            copy.start()
    for place in range(EARLY):
        drift_copy(place).start()
    per_slot = n_chunks * n_blocks

    def lend(places):
        for place in places:
            drift_copy(place).start()

    half = (LENT - EARLY) // 2
    evaluate(lent_items(range(EARLY, LENT)), {half * per_slot + LEAD + LAG: [functools.partial(lend, range(EARLY, EARLY + half))]})
    lend(range(EARLY + half, LENT))
    arrive(far[:AHEAD])
    for slot in far[:AHEAD]:
        prepare(slot)
    extras = {1: [functools.partial(arrive, far[AHEAD:])], (len(far) - AHEAD) * per_slot: [functools.partial(arrive, near)]}
    for place, slot in enumerate(far[AHEAD:]):
        extras.setdefault(place * per_slot + 2, []).append(functools.partial(prepare, slot))
    rest = AHEAD * per_slot
    for place, slot in enumerate(near):
        extras.setdefault(min((len(far) - AHEAD) * per_slot + 1 + place * rest // len(near), len(far) * per_slot - 1), []).append(functools.partial(prepare, slot))
    evaluate(first_items(far), extras)
    for slot in near:
        drift_arrival(slot).wait_recv()

    def integrate(chunk):
        last, x = drifts[slot_of(0), chunk], x_mine[:, columns(chunk)]
        for step in range(1, n_time):
            drift = drifts[slot_of(step), chunk]
            x = x + step_all[step - 1] * (0.5 * (last + drift))
            last = drift
            x_half[step] = x.astype(jnp.bfloat16)

    def out_copy(chunk, source, target):
        row, off = spot(source)
        cols = pl.ds(pl.multiple_of(off + chunk * CHUNK, CHUNK), CHUNK)
        return pltpu.make_async_remote_copy(
            src_ref=x_out.at[chunk, target], dst_ref=out_ref.at[row, :, cols], send_sem=out_send.at[chunk, target],
            recv_sem=out_recv.at[chunk, source], device_id={"time": target}, device_id_type=pl.DeviceIdType.MESH)

    def sweep_items(chunk, steps, state):
        def item(step):
            def put(drift):
                state["x"] = state["x"] + step_all[step - 1] * (0.5 * (state["last"] + drift))
                state["last"] = drift
                x_half[step] = state["x"].astype(jnp.bfloat16)
                x_out[chunk, step] = state["x"]
            return slot_of(step), lambda: x_half[step], put
        return [item(step) for step in steps]

    def initial(chunk):
        return {"last": drifts[slot_of(0), chunk], "x": x_mine[:, columns(chunk)]}

    def send(chunk, targets):
        for target in targets:
            @pl.when(me != target)
            def _():
                out_copy(chunk, me, target).start()

    def keep(chunk):
        @pl.when(me != 0)
        def _():
            out_ref[my_row, :, pl.ds(pl.multiple_of(my_off + chunk * CHUNK, CHUNK), CHUNK)] = x_out[chunk, me]

    later = SWEEPS - 1

    def sweep(index, carry):
        chunk = lax.div(index, later)
        evaluate(sweep_items(chunk, range(1, n_time), initial(chunk)))

        @pl.when(jnp.logical_and(lax.rem(index, later) == later - 1, chunk < n_chunks - 1))
        def _():
            send(chunk, range(1, n_time))
            keep(chunk)
            integrate(chunk + 1)
        return carry

    integrate(0)
    lax.fori_loop(0, n_chunks * later - 1, sweep, 0)
    final = n_chunks - 1
    state = initial(final)
    begin = 1
    for end in SEND_AFTER + (n_time,):
        evaluate(sweep_items(final, range(begin, end), state))
        send(final, range(begin, end))
        begin = end
    keep(final)

    for slot in near_first:
        for copy in mod_copies(me, peer_of(slot), slot):
            copy.wait_send()
    for place in range(LENT):
        drift_copy(place).wait_send()

    @pl.when(me == 0)
    def _():
        pltpu.make_async_copy(x_ref, out_ref, whole_sem.at[0]).wait()

    for chunk in range(n_chunks):
        for target in range(1, n_time):
            @pl.when(me != target)
            def _():
                out_copy(chunk, me, target).wait_send()

    @pl.when(me != 0)
    def _():
        for chunk in range(n_chunks):
            for dist in range(1, n_time):
                out_copy(chunk, lax.rem(me + dist, n_time), me).wait_recv()


def solution(mesh):
    n_time = mesh.shape["time"]

    def local(x_init, w_in, w_out, mod_scale, mod_shift, step_size):
        batch, tokens, channels = x_init.shape
        hidden = w_in.shape[1]
        mine = batch * tokens // n_time
        n_chunks = mine // CHUNK
        out = pl.pallas_call(
            functools.partial(kernel_body, n_time),
            out_shape=jax.ShapeDtypeStruct((batch, channels, tokens), jnp.float32),
            in_specs=[pl.BlockSpec(memory_space=pltpu.HBM)] * 6,
            out_specs=pl.BlockSpec(memory_space=pltpu.VMEM),
            scratch_shapes=[
                pltpu.VMEM((channels, hidden), jnp.bfloat16),
                pltpu.VMEM((channels, hidden), jnp.bfloat16),
                pltpu.SMEM((1,), jnp.float32),
                pltpu.VMEM((1, hidden), jnp.bfloat16),
                pltpu.VMEM((1, hidden), jnp.bfloat16),
                pltpu.VMEM((n_time, 2, hidden), jnp.bfloat16),
                pltpu.VMEM((n_time, 1, CHUNK), jnp.float32),
                pltpu.VMEM((n_time, hidden, 4 * channels), jnp.bfloat16),
                pltpu.VMEM((channels, mine), jnp.float32),
                pltpu.VMEM((batch, channels, tokens), jnp.float32),
                pltpu.VMEM((n_time, channels, CHUNK), jnp.bfloat16),
                pltpu.VMEM((n_time, n_chunks, channels, CHUNK), jnp.float32),
                pltpu.VMEM((LENT, n_chunks, channels, CHUNK), jnp.float32),
                pltpu.VMEM((n_chunks, n_time, channels, CHUNK), jnp.float32),
                pltpu.SemaphoreType.DMA((7,)),
                pltpu.SemaphoreType.DMA((1,)),
                pltpu.SemaphoreType.DMA((2, n_time)),
                pltpu.SemaphoreType.DMA((2, n_time)),
                pltpu.SemaphoreType.DMA((LENT,)),
                pltpu.SemaphoreType.DMA((n_time,)),
                pltpu.SemaphoreType.DMA((n_chunks, n_time)),
                pltpu.SemaphoreType.DMA((n_chunks, n_time)),
            ],
            compiler_params=pltpu.CompilerParams(collective_id=0, has_side_effects=True, vmem_limit_bytes=48 * 2**20),
            name="picard",
        )(*(pltpu.with_memory_space_constraint(a, pltpu.HBM) for a in (jnp.swapaxes(x_init, 1, 2), w_in, w_out.T, mod_scale, mod_shift)), step_size)
        return jnp.swapaxes(out, 1, 2)[None]

    return jax.shard_map(local, mesh=mesh, in_specs=(P("data"), P(), P(), P("time"), P("time"), P("time")), out_specs=P("time", "data"), check_vma=False)
```

```python
import functools

import jax
import jax.numpy as jnp
from jax import lax
from jax.experimental import pallas as pl
from jax.experimental.pallas import tpu as pltpu
from jax.sharding import PartitionSpec as P

SWEEPS = 4
TANH_LIN = 0.7978845608028654
TANH_CUB = TANH_LIN * 0.044715
CHUNK = 256
BLOCK = 384
LEAD = 1
LAG = 1
SEND_AFTER = (4, 8, 11, 13, 14)
LENT = 9
EARLY = 2
AHEAD = 2


def half_gelu_arg(half):
    square = half * half
    poly = square * (8.0 * TANH_CUB) + 2.0 * TANH_LIN
    gate = jnp.tanh(half * poly)
    return (half * (1.0 + gate)).astype(jnp.bfloat16)


def kernel_body(n_time, x_ref, w_in_ref, w_out_ref, scale_ref, shift_ref, step_ref, out_ref,
                w_in, w_out, step_own, scale_own, shift_own, mods_all, step_all, weights, x_mine, x_whole, x_half, drifts, drift_out, x_out, landed,
                local_sem, whole_sem, mod_send, mod_recv, drift_send, drift_recv, out_send, out_recv):
    me = lax.axis_index("time")
    channels, hidden = w_in.shape
    batch, _, tokens = x_ref.shape
    mine = batch * tokens // n_time
    per_row = tokens // mine
    n_chunks = mine // CHUNK
    n_blocks = hidden // BLOCK
    n_chips = n_time // 2

    def spot(device):
        return lax.div(device, per_row), lax.rem(device, per_row) * mine

    my_row, my_off = spot(me)
    fetches = [
        pltpu.make_async_copy(src, dst, local_sem.at[slot])
        for slot, (src, dst) in enumerate((
            (scale_ref, scale_own), (shift_ref, shift_own), (step_ref, step_own), (w_in_ref, w_in), (w_out_ref, w_out),
            (x_ref.at[my_row, :, pl.ds(pl.multiple_of(my_off, mine), mine)], x_mine), (x_ref, x_whole)))
    ]
    for fetch in fetches:
        fetch.start()

    chip, core = lax.div(me, 2), lax.rem(me, 2)

    def peer_of(slot):
        return lax.rem(chip + slot // 2, n_chips) * 2 + lax.rem(core + slot % 2, 2)

    def slot_of(step):
        return lax.rem(step // 2 + n_chips - chip, n_chips) * 2 + lax.rem(step % 2 + 2 - core, 2)

    groups = [[1]]
    for dist in range(1, n_chips // 2 + 1):
        ways = (dist,) if 2 * dist == n_chips else (dist, n_chips - dist)
        groups.append([way * 2 + other for way in ways for other in range(2)])
    near_first = [slot for group in groups for slot in group]

    barrier = pltpu.get_barrier_semaphore()
    for slot in reversed(near_first):
        pl.semaphore_signal(barrier, inc=1, device_id={"time": peer_of(slot)}, device_id_type=pl.DeviceIdType.MESH)
    for fetch in fetches:
        fetch.wait()
    mods_all[me] = jnp.concatenate([scale_own[...], shift_own[...]], axis=0)
    step_all[me] = jnp.full(step_all.shape[1:], step_own[0], jnp.float32)

    @pl.when(me == 0)
    def _():
        pltpu.make_async_copy(x_ref, landed.at[pl.ds(0, batch)], whole_sem.at[0]).start()

    def mod_copies(source, target, slot):
        return [
            pltpu.make_async_remote_copy(src_ref=ref.at[source], dst_ref=ref.at[source], send_sem=mod_send.at[kind, slot], recv_sem=mod_recv.at[kind, source],
                                         device_id={"time": target}, device_id_type=pl.DeviceIdType.MESH)
            for kind, ref in enumerate((mods_all, step_all))
        ]

    def prepare(slot):
        mods = mods_all[peer_of(slot)].astype(jnp.float32)
        folded = w_in[...].astype(jnp.float32) * (0.5 * (1.0 + mods[0:1]))
        high = folded.astype(jnp.bfloat16).astype(jnp.float32)
        rest = folded - high
        middle = rest.astype(jnp.bfloat16).astype(jnp.float32)
        low = rest - middle
        first_row = lax.broadcasted_iota(jnp.int32, (channels, hidden), 0) == 0
        bias = jnp.where(first_row, jnp.broadcast_to(0.5 * mods[1:2], (channels, hidden)), 0.0)
        stack = jnp.concatenate([high, middle, low, bias], axis=0)
        weights[slot] = stack.T.astype(jnp.bfloat16)

    ones = jnp.ones((channels, CHUNK), jnp.bfloat16)

    def evaluate(items, extras=None):
        extras = extras or {}
        blocks = [(item, block) for item in range(len(items)) for block in range(n_blocks)]
        stacked, pre, act, drift = {}, {}, {}, {}

        def project(index):
            item, block = blocks[index]
            slot, get_x, _ = items[item]
            if item not in stacked:
                x = get_x()
                stacked[item] = jnp.concatenate([x, x, x, ones], axis=0)
            pre[index] = jnp.dot(weights[slot, block * BLOCK:(block + 1) * BLOCK, :], stacked[item], preferred_element_type=jnp.float32)

        def contract(index):
            item, block = blocks[index]
            part = jnp.dot(w_out[:, block * BLOCK:(block + 1) * BLOCK], act.pop(index), preferred_element_type=jnp.float32)
            drift[item] = part if block == 0 else drift[item] + part
            if block == n_blocks - 1:
                items[item][2](drift.pop(item))

        for index in range(len(blocks) + LEAD + LAG + 1):
            for extra in extras.get(index, ()):
                extra()
            if index < len(blocks):
                project(index)
            if LEAD <= index < len(blocks) + LEAD:
                act[index - LEAD] = half_gelu_arg(pre.pop(index - LEAD))
            if LEAD + LAG <= index < len(blocks) + LEAD + LAG:
                contract(index - LEAD - LAG)

    def columns(chunk):
        return pl.ds(pl.multiple_of(chunk * CHUNK, CHUNK), CHUNK)

    def first_items(slots):
        def item(slot, chunk):
            def put(drift):
                drifts[slot, chunk] = drift
            return slot, lambda: x_mine[:, columns(chunk)].astype(jnp.bfloat16), put
        return [item(slot, chunk) for slot in slots for chunk in range(n_chunks)]

    def lent_items(places):
        def item(place, chunk):
            row, off = spot(peer_of(near_first[place]))
            def get():
                return x_whole[row, :, pl.ds(pl.multiple_of(off + chunk * CHUNK, CHUNK), CHUNK)].astype(jnp.bfloat16)
            def put(drift):
                drift_out[place, chunk] = drift
            return 0, get, put
        return [item(place, chunk) for place in places for chunk in range(n_chunks)]

    def drift_copy(place):
        slot = near_first[place]
        back = (n_chips - slot // 2) % n_chips * 2 + slot % 2
        return pltpu.make_async_remote_copy(
            src_ref=drift_out.at[place], dst_ref=drifts.at[back], send_sem=drift_send.at[place], recv_sem=drift_recv.at[back],
            device_id={"time": peer_of(slot)}, device_id_type=pl.DeviceIdType.MESH)

    def drift_arrival(slot):
        return pltpu.make_async_remote_copy(
            src_ref=drift_out.at[0], dst_ref=drifts.at[slot], send_sem=drift_send.at[0], recv_sem=drift_recv.at[slot],
            device_id={"time": peer_of(slot)}, device_id_type=pl.DeviceIdType.MESH)

    def arrive(slots):
        for slot in slots:
            for copy in mod_copies(peer_of(slot), peer_of(slot), slot):
                copy.wait_recv()

    prepare(0)
    evaluate(first_items([0]) + lent_items(range(EARLY)))
    pl.semaphore_wait(barrier, n_time - 1)
    far, near = near_first[LENT:], near_first[:LENT]
    for slot in far + near:
        for copy in mod_copies(me, peer_of(slot), slot):
            copy.start()
    for place in range(EARLY):
        drift_copy(place).start()
    per_slot = n_chunks * n_blocks

    def lend(places):
        for place in places:
            drift_copy(place).start()

    half = (LENT - EARLY) // 2
    evaluate(lent_items(range(EARLY, LENT)), {half * per_slot + LEAD + LAG: [functools.partial(lend, range(EARLY, EARLY + half))]})
    lend(range(EARLY + half, LENT))
    arrive(far[:AHEAD])
    for slot in far[:AHEAD]:
        prepare(slot)
    extras = {1: [functools.partial(arrive, far[AHEAD:])], (len(far) - AHEAD) * per_slot: [functools.partial(arrive, near)]}
    for place, slot in enumerate(far[AHEAD:]):
        extras.setdefault(place * per_slot + 2, []).append(functools.partial(prepare, slot))
    rest = AHEAD * per_slot
    for place, slot in enumerate(near):
        extras.setdefault(min((len(far) - AHEAD) * per_slot + 1 + place * rest // len(near), len(far) * per_slot - 1), []).append(functools.partial(prepare, slot))
    evaluate(first_items(far), extras)
    for slot in near:
        drift_arrival(slot).wait_recv()

    def integrate(chunk):
        last, x = drifts[slot_of(0), chunk], x_mine[:, columns(chunk)]
        for step in range(1, n_time):
            drift = drifts[slot_of(step), chunk]
            x = x + step_all[step - 1] * (0.5 * (last + drift))
            last = drift
            x_half[step] = x.astype(jnp.bfloat16)

    def out_copy(chunk, source, target):
        row, off = spot(source)
        cols = pl.ds(pl.multiple_of(off + chunk * CHUNK, CHUNK), CHUNK)
        own = source == target
        return pltpu.make_async_remote_copy(
            src_ref=x_out.at[chunk, target], dst_ref=landed.at[jnp.where(own, batch, row), :, cols], send_sem=out_send.at[chunk, target],
            recv_sem=out_recv.at[chunk, jnp.where(own, n_time, source)], device_id={"time": jnp.where(own, target + 1 - 2 * lax.rem(target, 2), target)},
            device_id_type=pl.DeviceIdType.MESH)

    def sweep_items(chunk, steps, state):
        def item(step):
            def put(drift):
                state["x"] = state["x"] + step_all[step - 1] * (0.5 * (state["last"] + drift))
                state["last"] = drift
                x_half[step] = state["x"].astype(jnp.bfloat16)
                x_out[chunk, step] = state["x"]
            return slot_of(step), lambda: x_half[step], put
        return [item(step) for step in steps]

    def initial(chunk):
        return {"last": drifts[slot_of(0), chunk], "x": x_mine[:, columns(chunk)]}

    def send(chunk, target):
        out_copy(chunk, me, target).start()

    def keep(chunk):
        @pl.when(me != 0)
        def _():
            landed[my_row, :, pl.ds(pl.multiple_of(my_off + chunk * CHUNK, CHUNK), CHUNK)] = x_out[chunk, me]

    later = SWEEPS - 1

    def sweep(index, carry):
        chunk = lax.div(index, later)
        evaluate(sweep_items(chunk, range(1, n_time), initial(chunk)))

        @pl.when(jnp.logical_and(lax.rem(index, later) == later - 1, chunk < n_chunks - 1))
        def _():
            for target in range(1, n_time):
                send(chunk, target)
            keep(chunk)
            integrate(chunk + 1)
        return carry

    integrate(0)
    lax.fori_loop(0, n_chunks * later - 1, sweep, 0)
    final = n_chunks - 1
    sends, begin = {}, 1
    for end in SEND_AFTER + (n_time - 1,):
        sends[end * n_blocks + LEAD + LAG] = [functools.partial(send, final, target) for target in range(begin, end + 1)]
        begin = end + 1
    evaluate(sweep_items(final, range(1, n_time), initial(final)), sends)
    keep(final)

    for slot in near_first:
        for copy in mod_copies(me, peer_of(slot), slot):
            copy.wait_send()
    for place in range(LENT):
        drift_copy(place).wait_send()

    @pl.when(me == 0)
    def _():
        pltpu.make_async_copy(x_ref, landed.at[pl.ds(0, batch)], whole_sem.at[0]).wait()

    for chunk in range(n_chunks):
        for target in range(1, n_time):
            out_copy(chunk, me, target).wait_send()

    @pl.when(me != 1)
    def _():
        for chunk in range(n_chunks):
            pair = me + 1 - 2 * lax.rem(me, 2)
            out_copy(chunk, pair, pair).wait_recv()

    @pl.when(me != 0)
    def _():
        for chunk in range(n_chunks):
            for dist in range(1, n_time):
                out_copy(chunk, lax.rem(me + dist, n_time), me).wait_recv()

    out_ref[...] = landed[0:batch]


def solution(mesh):
    n_time = mesh.shape["time"]

    def local(x_init, w_in, w_out, mod_scale, mod_shift, step_size):
        batch, tokens, channels = x_init.shape
        hidden = w_in.shape[1]
        mine = batch * tokens // n_time
        n_chunks = mine // CHUNK
        out = pl.pallas_call(
            functools.partial(kernel_body, n_time),
            out_shape=jax.ShapeDtypeStruct((batch, channels, tokens), jnp.float32),
            in_specs=[pl.BlockSpec(memory_space=pltpu.HBM)] * 6,
            out_specs=pl.BlockSpec(memory_space=pltpu.VMEM),
            scratch_shapes=[
                pltpu.VMEM((channels, hidden), jnp.bfloat16),
                pltpu.VMEM((channels, hidden), jnp.bfloat16),
                pltpu.SMEM((1,), jnp.float32),
                pltpu.VMEM((1, hidden), jnp.bfloat16),
                pltpu.VMEM((1, hidden), jnp.bfloat16),
                pltpu.VMEM((n_time, 2, hidden), jnp.bfloat16),
                pltpu.VMEM((n_time, 1, CHUNK), jnp.float32),
                pltpu.VMEM((n_time, hidden, 4 * channels), jnp.bfloat16),
                pltpu.VMEM((channels, mine), jnp.float32),
                pltpu.VMEM((batch, channels, tokens), jnp.float32),
                pltpu.VMEM((n_time, channels, CHUNK), jnp.bfloat16),
                pltpu.VMEM((n_time, n_chunks, channels, CHUNK), jnp.float32),
                pltpu.VMEM((LENT, n_chunks, channels, CHUNK), jnp.float32),
                pltpu.VMEM((n_chunks, n_time, channels, CHUNK), jnp.float32),
                pltpu.VMEM((batch + 1, channels, tokens), jnp.float32),
                pltpu.SemaphoreType.DMA((7,)),
                pltpu.SemaphoreType.DMA((1,)),
                pltpu.SemaphoreType.DMA((2, n_time)),
                pltpu.SemaphoreType.DMA((2, n_time)),
                pltpu.SemaphoreType.DMA((LENT,)),
                pltpu.SemaphoreType.DMA((n_time,)),
                pltpu.SemaphoreType.DMA((n_chunks, n_time)),
                pltpu.SemaphoreType.DMA((n_chunks, n_time + 1)),
            ],
            compiler_params=pltpu.CompilerParams(collective_id=0, has_side_effects=True, vmem_limit_bytes=48 * 2**20),
            name="picard",
        )(*(pltpu.with_memory_space_constraint(a, pltpu.HBM) for a in (jnp.swapaxes(x_init, 1, 2), w_in, w_out.T, mod_scale, mod_shift)), step_size)
        return jnp.swapaxes(out, 1, 2)[None]

    return jax.shard_map(local, mesh=mesh, in_specs=(P("data"), P(), P(), P("time"), P("time"), P("time")), out_specs=P("time", "data"), check_vma=False)
```
